32 devices in a mesh: src: 16 (over z, y, core), sub: 2 (over x).
Axes of the slice: x: 2, y: 2, z: 4, core: 2. Of those that a mesh axis runs over, the one named last changes fastest.
Arguments:
- child_rhs: float32 [2, 1024, 4096], P('sub', None, 'src'), may hold values from -6 to 6
- root_rhs: float32 [2048, 4096], P('sub', 'src'), may hold values from -6 to 6
- child_inverse: bfloat16 [2, 1024, 1024], P('sub', 'src'), as said below
- coupling_block: bfloat16 [2, 1024, 1024], P('sub', 'src'), may hold values from -0.1875 to 0.1875
- root_inverse: bfloat16 [2048, 2048], P('sub', 'src'), as said below
- child_orders: int32 [2], P('sub'), may hold values from 716 to 1024, as said below
- coupling_rows: int32 [2, 1024], P('sub'), may hold values from 0 to 2047, as said below
Outputs:
- child_solution: float32 [2, 1024, 4096], P('sub', None, 'src')
- root_solution: float32 [2048, 4096], P('sub', 'src')
The draws below stay inside these ranges and needn't reach their ends.
Inputs may be any that keep to these rules, and one draw needn't show every extreme that they name: Each child_inverse[j] is lower triangular: zero above the diagonal, diagonal entries between 0.8 and 1.25. `root_inverse`: lower triangular: zero above the diagonal, diagonal entries between 0.8 and 1.25. `coupling_rows`: each row holds 1024 distinct root rows in increasing order. `child_orders`: some child has order 1024.
All inputs are finite; a program needn't handle non-finite values.
Results may differ from the reference program's by a relative error of at most 0.0093.
Values may be sent and summed in bfloat16 or wider, within the bound.
A program may use at most 64 MiB of HBM per device.

```python
import math
import jax
import jax.numpy as jnp

S0 = 2048
S1 = 1024
K = 1024
CHILDREN = 2
SOURCES = 4096


def lower_factor(key, batch_count, matrix_order):
    key_off, key_diag = jax.random.split(key)
    spread = jnp.clip(jax.random.normal(key_off, (batch_count, matrix_order, matrix_order), jnp.float32), -6.0, 6.0)
    diagonal = jax.random.uniform(key_diag, (batch_count, matrix_order), jnp.float32, 0.8, 1.25)
    positions = jnp.arange(matrix_order)
    strict_lower = positions[:, None] > positions[None, :]
    on_diagonal = positions[:, None] == positions[None, :]
    factor = jnp.where(strict_lower, spread * (0.5 / math.sqrt(matrix_order)), 0.0)
    return factor + jnp.where(on_diagonal, diagonal[:, :, None], 0.0)


def draw_child_inverse(key, part):
    return lower_factor(jax.random.fold_in(key, 11), CHILDREN, S1).astype(jnp.bfloat16)


def draw_root_inverse(key, part):
    return lower_factor(jax.random.fold_in(key, 12), 1, S0)[0].astype(jnp.bfloat16)


def draw_coupling_rows(key, part):

    def choose_rows(child_number):
        shuffled = jax.random.permutation(jax.random.fold_in(jax.random.fold_in(key, 13), child_number), S0)
        return jnp.sort(shuffled[:K])
    return jax.vmap(choose_rows)(jnp.arange(CHILDREN)).astype(jnp.int32)


def draw_child_orders(key, part):
    orders = jax.random.randint(jax.random.fold_in(key, 14), (CHILDREN,), 7 * S1 // 10, S1 + 1, jnp.int32)
    largest = jax.random.randint(jax.random.fold_in(key, 15), (), 0, CHILDREN, jnp.int32)
    return jnp.where(jnp.arange(CHILDREN, dtype=jnp.int32) == largest, S1, orders).astype(jnp.int32)


def block_levels(rng, extent, cuts, smallest, high):
    def one(dim, shards_of):
        heights = jax.random.uniform(jax.random.fold_in(jax.random.fold_in(rng, 6), dim), (shards_of,), jnp.float32, smallest / len(cuts), high / len(cuts))
        return jnp.repeat(jnp.exp(heights), extent[dim] // shards_of).reshape((-1,) + (1,) * (len(extent) - dim - 1))

    loudness = one(*cuts[0])
    for cut in cuts[1:]:
        loudness = loudness * one(*cut)
    return loudness


def bell_draw(stream_key, shape, scale, limit, shards=(), held_as=jnp.bfloat16):
    values = scale * jax.random.normal(stream_key, shape, jnp.float32)
    if shards:
        values = values * block_levels(stream_key, shape, shards, -0.22, 0.18)
    return jnp.clip(values, -limit, limit).astype(held_as)


def setup_inputs(seed: int = 0) -> dict:
    keys = jax.random.split(jax.random.key(seed), 8)
    return {
        "child_rhs": bell_draw(keys[0], (CHILDREN, S1, SOURCES), 1.0, 6.0, ((0, 2), (2, 16)), jnp.float32),
        "root_rhs": bell_draw(keys[1], (S0, SOURCES), 1.0, 6.0, ((0, 2), (1, 16)), jnp.float32),
        "child_inverse": draw_child_inverse(jax.random.fold_in(keys[7], 71), 0),
        "coupling_block": bell_draw(keys[3], (CHILDREN, K, S1), S1 ** -0.5, 0.1875, ((0, 2), (1, 16))),
        "root_inverse": draw_root_inverse(jax.random.fold_in(keys[7], 71), 0),
        "child_orders": draw_child_orders(jax.random.fold_in(keys[7], 71), 0),
        "coupling_rows": draw_coupling_rows(jax.random.fold_in(keys[7], 71), 0),
    }


def reference(child_rhs, root_rhs, child_inverse, coupling_block, root_inverse, child_orders, coupling_rows):
    positions = jnp.arange(S1, dtype=jnp.int32)
    update_total = jnp.zeros(root_rhs.shape, jnp.float32)
    solved_list = []
    for child in range(CHILDREN):
        alive = (positions < child_orders[child])[:, None]
        child_source = jnp.where(alive, child_rhs[child], 0.0).astype(jnp.bfloat16)
        solved = jnp.where(alive, jnp.dot(child_inverse[child], child_source, preferred_element_type=jnp.float32), 0.0)
        solved_list.append(solved)
        update = jnp.dot(coupling_block[child], solved.astype(jnp.bfloat16), preferred_element_type=jnp.float32)
        update_total = update_total.at[coupling_rows[child]].add(update)
    root_source = (root_rhs - update_total).astype(jnp.bfloat16)
    root_forward = jnp.dot(root_inverse, root_source, preferred_element_type=jnp.float32)
    root_round = root_forward.astype(jnp.bfloat16)
    root_solution = jnp.dot(root_inverse.T, root_round, preferred_element_type=jnp.float32)
    root_half = root_solution.astype(jnp.bfloat16)
    result_list = []
    for child in range(CHILDREN):
        alive = (positions < child_orders[child])[:, None]
        picked = root_half[coupling_rows[child]]
        pulled = jnp.dot(coupling_block[child].T, picked, preferred_element_type=jnp.float32)
        residue = jnp.where(alive, solved_list[child] - pulled, 0.0).astype(jnp.bfloat16)
        result = jnp.dot(child_inverse[child].T, residue, preferred_element_type=jnp.float32)
        result_list.append(jnp.where(alive, result, 0.0))
    return jnp.stack(result_list), root_solution
```

```python
import functools
import jax
import jax.numpy as jnp
from jax import lax
from jax.experimental import pallas as pl
from jax.experimental.pallas import tpu as pltpu
from jax.sharding import PartitionSpec as P

MESH = pl.DeviceIdType.MESH
F32 = jnp.float32
BF16 = jnp.bfloat16


def dot_t(left, right):
    return lax.dot_general(left, right, (((1,), (1,)), ((), ())), preferred_element_type=F32)


def dot_n(left, right):
    return jnp.dot(left, right, preferred_element_type=F32)


def kernel(
    lines, rhs_ref, rrhs_ref, inv_ref, cpl_ref, rinv_ref, order_ref, rows_ref, child_out, root_out,
    inv, cpl, root, hot, src_t, solved_t, upd_t, placed_t, give, take, rr_t, sol_t, sol_b, res_t,
    recv, swap_s, send_z, send_y, send_x, send_c, ex_s, ex_r, bk_s, bk_r, lay,
):
    me, x = lax.axis_index("src"), lax.axis_index("sub")
    core, y, z = me % 2, (me // 2) % 2, me // 4
    strip = inv_ref.shape[0]
    order = inv_ref.shape[1]
    width = rinv_ref.shape[1]
    part = root.shape[1]
    half = order // 2
    cols = rhs_ref.shape[1]
    hcols = cols // 2
    own_rows = rrhs_ref.shape[0]
    blocks = root.shape[0]
    tile = 256
    here = pl.multiple_of(x * hcols, hcols)
    there = pl.multiple_of((1 - x) * hcols, hcols)

    def src_of(zz, yy, cc):
        return (zz * 2 + yy) * 2 + cc

    def dev(zz, yy, cc, xx):
        return {"src": src_of(zz, yy, cc), "sub": xx}

    barrier = pltpu.get_barrier_semaphore()

    def hello(device):
        pl.semaphore_signal(barrier, inc=1, device_id=device, device_id_type=MESH)

    hello(dev(z, 1 - y, core, x))
    hello(dev(z, y, 1 - core, x))
    hello(dev(z, y, core, 1 - x))

    @pl.when(z > 0)
    def _():
        hello(dev(z - 1, y, core, x))

    @pl.when(z < lines - 1)
    def _():
        hello(dev(z + 1, y, core, x))

    inner = jnp.logical_and(z > 0, z < lines - 1)
    pl.when(inner)(lambda: pl.semaphore_wait(barrier, 5))
    pl.when(jnp.logical_not(inner))(lambda: pl.semaphore_wait(barrier, 4))

    kept = 2 * x
    given = 3 - 2 * x
    swapped = 2 * x + 1
    kept_far = 2 - 2 * x
    given_far = 1 + 2 * x

    def strip_ref(which, s):
        r = pl.multiple_of(s * strip, strip)
        return (inv if which == 0 else cpl).at[pl.ds(r, strip), :]

    def block_ref(b, s):
        return root.at[b, :, pl.ds(pl.multiple_of(s * width, width), width)]

    def lives(b, s):
        return s * width < (b + 1) * part

    def views(which, b, s):
        if which == 0:
            ref = strip_ref(0, s)
            r = pl.multiple_of(s * strip, strip)
            narrow = (s + 1) * strip <= half
            return [(narrow, inv.at[pl.ds(r, strip), pl.ds(0, half)]), (jnp.logical_not(narrow), ref)]
        if which == 1:
            return [(None, strip_ref(1, s))]
        return [(lives(b, s), block_ref(b, s))]

    def under(cond, f):
        if cond is None:
            f()
        else:
            pl.when(cond)(f)

    def rsem(which, b, s):
        return recv.at[which if which < 2 else b + 2, s]

    def push(which, b, s, sem, device, wait=False):
        for cond, ref in views(which, b, s):
            def f(ref=ref):
                cp = pltpu.make_async_remote_copy(
                    src_ref=ref, dst_ref=ref, send_sem=sem, recv_sem=rsem(which, b, s),
                    device_id=device, device_id_type=MESH,
                )
                if wait:
                    cp.wait_send()
                else:
                    cp.start()
            under(cond, f)

    def arrive(which, b, s):
        for cond, ref in views(which, b, s):
            def f(ref=ref):
                pltpu.make_async_remote_copy(
                    src_ref=ref, dst_ref=ref, send_sem=recv.at[0, 0], recv_sem=rsem(which, b, s),
                    device_id=dev(z, y, 1 - core, x), device_id_type=MESH,
                ).wait_recv()
            under(cond, f)

    def sends(cls, which, b, zz, far, wait):
        yy = jnp.where(far, 1 - y, y) if not isinstance(far, bool) else (1 - y if far else y)
        s = src_of(zz, yy, core)
        if not far:
            @pl.when(jnp.logical_and(zz <= z, z < lines - 1))
            def _():
                push(which, b, s, send_z.at[cls, 0, zz], dev(z + 1, y, core, x), wait)

            @pl.when(jnp.logical_and(zz >= z, z > 0))
            def _():
                push(which, b, s, send_z.at[cls, 1, zz], dev(z - 1, y, core, x), wait)

            push(which, b, s, send_y.at[cls, zz], dev(z, 1 - y, core, x), wait)
        if which == 2:
            push(which, b, s, send_x.at[cls - 2, int(far), zz], dev(z, y, core, 1 - x), wait)
        push(which, b, s, send_c.at[cls, int(far), zz], dev(z, y, 1 - core, x), wait)

    def own(cls, which, b):
        sends(cls, which, b, z, False, False)

    def relay(cls, which, b, far):
        def step(k, _):
            zz = z + ((k + 1) // 2) * (1 - 2 * (k % 2))

            @pl.when(jnp.logical_and(zz >= 0, zz < lines))
            def _():
                arrive(which, b, src_of(zz, 1 - y if far else y, core))
                sends(cls, which, b, zz, far, False)
            return 0
        lax.fori_loop(0 if far else 1, 2 * lines - 1, step, 0)

    def over_core(which, b):
        def step(k, _):
            arrive(which, b, src_of(k // 2, k % 2, 1 - core))
            return 0
        lax.fori_loop(0, 2 * lines, step, 0)

    def far_plane(cls, b):
        def step(k, _):
            s = src_of(k // 2, k % 2, core)
            arrive(2, b, s)
            push(2, b, s, send_c.at[cls, k % 2, k // 2], dev(z, y, 1 - core, x))
            return 0
        lax.fori_loop(0, 2 * lines, step, 0)

    def swap():
        return pltpu.make_async_remote_copy(
            src_ref=rinv_ref.at[pl.ds(part, part), :], dst_ref=block_ref(swapped, me),
            send_sem=swap_s, recv_sem=recv.at[2 + swapped, me],
            device_id=dev(z, y, core, 1 - x), device_id_type=MESH,
        )

    placing = [
        pltpu.make_async_copy(inv_ref, strip_ref(0, me), lay.at[0]),
        pltpu.make_async_copy(cpl_ref, strip_ref(1, me), lay.at[1]),
        pltpu.make_async_copy(rinv_ref.at[pl.ds(0, part), :], block_ref(kept, me), lay.at[2]),
    ]
    for copy in placing:
        copy.start()
    pl.when(lives(swapped, me))(lambda: swap().start())

    for copy in placing:
        copy.wait()
    own(0, 0, None)
    own(1, 1, None)

    index = rows_ref[...]

    @pl.loop(0, hot.shape[0] // tile)
    def _(i):
        r = pl.multiple_of(i * tile, tile)
        at = lax.broadcasted_iota(jnp.int32, (tile, index.shape[1]), 0) + r
        hot[pl.ds(r, tile), :] = jnp.where(at == index, 1.0, 0.0).astype(BF16)

    alive = lax.broadcasted_iota(jnp.int32, (1, order), 1) < order_ref[0]
    src_t[...] = jnp.where(alive, rhs_ref[...].T, 0.0).astype(BF16)
    own(2, 2, kept)
    relay(0, 0, None, False)
    pl.when(lives(given, me))(lambda: pltpu.make_async_remote_copy(
        src_ref=block_ref(given, me), dst_ref=block_ref(given, me), send_sem=swap_s,
        recv_sem=recv.at[2 + given, me], device_id=dev(z, y, core, 1 - x), device_id_type=MESH,
    ).wait_recv())
    relay(0, 0, None, True)
    relay(1, 1, None, False)
    own(3, 2, given)
    over_core(0, None)
    low = pl.ds(0, half)
    high = pl.ds(half, half)
    solved_t[:, low] = jnp.where(alive[:, :half], dot_t(src_t[:, low], inv[low, low]), 0.0)
    solved_t[:, high] = jnp.where(alive[:, half:], dot_t(src_t[...], inv[high, :]), 0.0)
    relay(1, 1, None, True)
    relay(2, 2, kept, False)
    over_core(1, None)
    upd_t[...] = dot_t(solved_t[...].astype(BF16), cpl[...]).astype(BF16)

    @pl.loop(0, placed_t.shape[1] // tile)
    def _(i):
        r = pl.multiple_of(i * tile, tile)
        placed_t[:, pl.ds(r, tile)] = -dot_t(upd_t[...], hot[pl.ds(r, tile), :])

    mine = pl.ds(pl.multiple_of(x * own_rows, own_rows), own_rows)
    placed_t[:, mine] += rrhs_ref[...].T
    give[...] = placed_t[pl.ds(there, hcols), :].astype(BF16)
    relay(2, 2, kept, True)

    def exchange():
        return pltpu.make_async_remote_copy(
            src_ref=give, dst_ref=take, send_sem=ex_s, recv_sem=ex_r,
            device_id=dev(z, y, core, 1 - x), device_id_type=MESH,
        )

    exchange().start()
    relay(3, 2, given, False)
    relay(3, 2, given, True)
    over_core(2, kept)
    over_core(2, given)
    exchange().wait()
    take[...] = (placed_t[pl.ds(here, hcols), :] + take[...].astype(F32)).astype(BF16)
    far_plane(4, kept_far)
    far_plane(5, given_far)
    over_core(2, kept_far)
    over_core(2, given_far)
    for b in range(blocks):
        upto = pl.ds(0, (b + 1) * part)
        rr_t[:, pl.ds(b * part, part)] = dot_t(take[:, upto], root[b, :, upto]).astype(BF16)

    def back(a):
        piece = sol_b.at[pl.ds(here, hcols), pl.ds(a * part, part)]
        return pltpu.make_async_remote_copy(
            src_ref=piece, dst_ref=piece, send_sem=bk_s.at[a], recv_sem=bk_r.at[a],
            device_id=dev(z, y, core, 1 - x), device_id_type=MESH,
        )

    for a in reversed(range(blocks)):
        at = pl.ds(a * part, part)
        total = dot_n(rr_t[:, at], root[a, :, at])
        for b in range(a + 1, blocks):
            total += dot_n(rr_t[:, pl.ds(b * part, part)], root[b, :, at])
        sol_t[:, at] = total
        sol_b[pl.ds(here, hcols), at] = total.astype(BF16)
        if a + 1 < blocks:
            back(a + 1).start()

    def finish(first):
        rows = pl.ds(first, hcols)
        picked = dot_n(sol_b[rows, :], hot[...]).astype(BF16)
        pulled = dot_n(picked, cpl[...])
        res_t[rows, :] = jnp.where(alive, solved_t[rows, :] - pulled, 0.0).astype(BF16)
        first_half = dot_n(res_t[rows, :], inv[:, low])
        second_half = dot_n(res_t[rows, high], inv[high, high])
        solved_t[rows, low] = jnp.where(alive[:, :half], first_half, 0.0)
        solved_t[rows, high] = jnp.where(alive[:, half:], second_half, 0.0)

    back(0).start()
    finish(here)
    for a in range(blocks):
        back(a).wait_recv()
    finish(there)
    child_out[...] = solved_t[...].T
    src_t[...] = sol_b[:, mine]
    solved_t[...] = src_t[...].astype(F32)
    solved_t[pl.ds(here, hcols), :] = sol_t[:, mine]
    root_out[...] = solved_t[...].T

    pl.when(lives(swapped, me))(lambda: swap().wait_send())
    for a in range(blocks):
        back(a).wait_send()
    for cls, which, b in ((0, 0, None), (1, 1, None), (2, 2, kept), (3, 2, given)):
        for far in (False, True):
            def step(zz, _, cls=cls, which=which, b=b, far=far):
                sends(cls, which, b, zz, far, True)
                return 0
            lax.fori_loop(0, lines, step, 0)
    for cls, b in ((4, kept_far), (5, given_far)):
        def step(k, _, cls=cls, b=b):
            push(2, b, src_of(k // 2, k % 2, core), send_c.at[cls, k % 2, k // 2],
                 dev(z, y, 1 - core, x), True)
            return 0
        lax.fori_loop(0, 2 * lines, step, 0)


def fused(child_rhs, root_rhs, child_inverse, coupling_block, root_inverse, child_orders, coupling_rows):
    n = lax.axis_size("src")
    lines = n // 4
    order = child_inverse.shape[2]
    cols = child_rhs.shape[2]
    own_rows = root_rhs.shape[0]
    root_order = own_rows * lax.axis_size("sub")
    couples = coupling_block.shape[1] * n
    vmem = pl.BlockSpec(memory_space=pltpu.VMEM)
    smem = pl.BlockSpec(memory_space=pltpu.SMEM)
    dma = pltpu.SemaphoreType.DMA
    child_out, root_out = pl.pallas_call(
        functools.partial(kernel, lines),
        out_shape=(
            jax.ShapeDtypeStruct((order, cols), F32),
            jax.ShapeDtypeStruct((own_rows, cols), F32),
        ),
        in_specs=[vmem] * 5 + [smem, vmem],
        out_specs=(vmem, vmem),
        scratch_shapes=[
            pltpu.VMEM((order, order), BF16),
            pltpu.VMEM((couples, order), BF16),
            pltpu.VMEM((4, root_order // 4, root_order), BF16),
            pltpu.VMEM((root_order, couples), BF16),
            pltpu.VMEM((cols, order), BF16),
            pltpu.VMEM((cols, order), F32),
            pltpu.VMEM((cols, couples), BF16),
            pltpu.VMEM((cols, root_order), F32),
            pltpu.VMEM((cols // 2, root_order), BF16),
            pltpu.VMEM((cols // 2, root_order), BF16),
            pltpu.VMEM((cols // 2, root_order), BF16),
            pltpu.VMEM((cols // 2, root_order), F32),
            pltpu.VMEM((cols, root_order), BF16),
            pltpu.VMEM((cols, order), BF16),
            dma((6, n)),
            dma,
            dma((4, 2, lines)),
            dma((4, lines)),
            dma((2, 2, lines)),
            dma((6, 2, lines)),
            dma,
            dma,
            dma((4,)),
            dma((4,)),
            dma((3,)),
        ],
        compiler_params=pltpu.CompilerParams(
            collective_id=0, has_side_effects=True, vmem_limit_bytes=60 * 1024 * 1024
        ),
    )(child_rhs[0], root_rhs, child_inverse[0], coupling_block[0], root_inverse, child_orders, coupling_rows)
    return child_out[None], root_out


def contract_rows(left, right):
    return lax.dot_general(
        left, right, (((0,), (0,)), ((), ())), preferred_element_type=jnp.float32
    )


def on_device(
    child_rhs, root_rhs, child_inverse, coupling_block, root_inverse, child_orders, coupling_rows
):
    inverse = child_inverse[0]
    coupling = coupling_block[0]
    coupling_index = coupling_rows[0]
    columns = child_rhs.shape[2]
    child_order = inverse.shape[1]
    block_rows = root_rhs.shape[0]
    root_order = root_inverse.shape[1] * lax.axis_size("src")
    alive = (lax.iota(jnp.int32, child_order) < child_orders[0])[:, None]
    child_source = jnp.where(alive, child_rhs[0], 0.0).astype(jnp.bfloat16)
    forward = jnp.dot(
        lax.all_gather(inverse, "src", axis=0, tiled=True),
        child_source,
        preferred_element_type=jnp.float32,
    )
    child_solved = jnp.where(alive, forward, 0.0)
    solved_round = child_solved.astype(jnp.bfloat16)
    update = jnp.dot(
        lax.all_gather(coupling, "src", axis=0, tiled=True),
        solved_round,
        preferred_element_type=jnp.float32,
    )
    placed = jnp.zeros((root_order, columns), jnp.float32).at[coupling_index].add(update)
    first_row = lax.axis_index("sub") * block_rows
    own_rows = lax.dynamic_slice_in_dim(placed, first_row, block_rows, 0)
    summand = lax.dynamic_update_slice_in_dim(-placed, root_rhs - own_rows, first_row, 0)
    root_source = lax.psum(summand, "sub").astype(jnp.bfloat16)
    root_forward = jnp.dot(
        lax.all_gather(root_inverse, "src", axis=1, tiled=True),
        root_source,
        preferred_element_type=jnp.float32,
    )
    root_round = root_forward.astype(jnp.bfloat16)
    partial_root = contract_rows(
        lax.all_gather(root_inverse, "src", axis=1, tiled=True), root_round
    )
    root_out = lax.psum_scatter(partial_root, "sub", scatter_dimension=0, tiled=True)
    rounded_all = lax.all_gather(root_out.astype(jnp.bfloat16), "sub", axis=0, tiled=True)
    picked = rounded_all[coupling_index]
    pulled = contract_rows(lax.all_gather(coupling, "src", axis=0, tiled=True), picked)
    residue = jnp.where(alive, child_solved - pulled, 0.0).astype(jnp.bfloat16)
    backward = contract_rows(lax.all_gather(inverse, "src", axis=0, tiled=True), residue)
    child_out = jnp.where(alive, backward, 0.0)[None]
    return (child_out, root_out)


def route(child_rhs, root_rhs, child_inverse, *rest):
    n, subs = lax.axis_size("src"), lax.axis_size("sub")
    order = child_inverse.shape[2]
    fits = subs == 2 and n % 4 == 0 and n >= 8 and root_rhs.shape[0] == order == rest[0].shape[1] * n
    fits = fits and rest[1].shape[1] % 128 == 0 and child_rhs.shape[2] % 256 == 0
    form = fused if fits else on_device
    return form(child_rhs, root_rhs, child_inverse, *rest)


def solution(mesh):
    return jax.shard_map(
        route,
        mesh=mesh,
        in_specs=(
            P("sub", None, "src"),
            P("sub", "src"),
            P("sub", "src", None),
            P("sub", "src", None),
            P("sub", "src"),
            P("sub"),
            P("sub", None),
        ),
        out_specs=(P("sub", None, "src"), P("sub", "src")),
        check_vma=False,
    )
```
